32 devices in a mesh: row: 4 (over y, core), col: 8 (over z, x).
Axes of the slice: x: 2, y: 2, z: 4, core: 2. Of those that a mesh axis runs over, the one named last changes fastest.
Arguments:
- matrix_in: float32 [8, 2048, 4, 4096], P(None, 'row', None, 'col'), as said below
- panel_start: int32 [1], replicated, may hold values from 0 to 29
Outputs:
- matrix_out: float32 [8, 2048, 4, 4096], P(None, 'row', None, 'col')
The draws below stay inside these ranges and needn't reach their ends.
Inputs may be any that keep to these rules, and one draw needn't show every extreme that they name: matrix_in is symmetric and positive definite.
All inputs are finite; a program needn't handle non-finite values.
Results may differ from the reference program's by a relative error of at most 0.0001.
Values sent between devices are 32-bit elements.
A program may use at most 192 MiB of HBM per device.

```python
import jax
import jax.numpy as jnp
from jax import lax

ORDER = 16384
NB = 512
PANELS = 2
BLOCKS = 32
LOC_BR = 8
LOC_BC = 4


def draw_matrix_in(key, part):
    key_gen = jax.random.fold_in(key, 21)
    key_shift = jax.random.fold_in(key, 22)
    inner_count = max(2 * NB, ORDER // 16)
    generator = jax.random.truncated_normal(key_gen, -6.0, 6.0, (ORDER, inner_count), jnp.float32)
    shift = jax.random.uniform(key_shift, (ORDER,), jnp.float32, 0.4, 0.8)
    common = jnp.zeros((ORDER,), jnp.float32)
    scales = jnp.ones((ORDER,), jnp.float32)
    weight = 0.0
    gram = lax.dot_general(generator, generator, (((1,), (1,)), ((), ())), precision=lax.Precision.HIGHEST, preferred_element_type=jnp.float32)
    gram = gram * (1.0 / inner_count)
    gram = 0.5 * (gram + gram.T)
    matrix = gram + weight * common[:, None] * common[None, :] + jnp.diag(shift)
    matrix = scales[:, None] * matrix * scales[None, :]
    return matrix.reshape(LOC_BR, ORDER // LOC_BR, LOC_BC, ORDER // LOC_BC)


def setup_inputs(seed: int = 0) -> dict:
    arg_keys = jax.random.split(jax.random.key(seed), 3)
    matrix_in = draw_matrix_in(jax.random.fold_in(arg_keys[2], 71), 0)
    panel_start = jax.random.randint(arg_keys[1], (1,), 0, BLOCKS - 2).astype(jnp.int32)
    return dict(matrix_in=matrix_in, panel_start=panel_start)


def reference(matrix_in, panel_start):
    matrix = matrix_in.reshape(ORDER, ORDER)
    block_index = jnp.arange(ORDER, dtype=jnp.int32) // NB
    first_panel = panel_start[0].astype(jnp.int32)
    for panel_step in range(PANELS):
        panel = first_panel + panel_step
        offset = (panel * NB).astype(jnp.int32)
        zero_index = jnp.zeros((), jnp.int32)
        diag_block = lax.dynamic_slice(matrix, (offset, offset), (NB, NB))
        factor = jnp.linalg.cholesky(diag_block)
        column_strip = lax.dynamic_slice(matrix, (zero_index, offset), (ORDER, NB))
        solved = jax.scipy.linalg.solve_triangular(factor, column_strip.T, lower=True).T
        below_panel = (block_index > panel)[:, None]
        column = jnp.where(below_panel, solved, jnp.float32(0.0))
        product = lax.dot_general(column.astype(jnp.float32), column.astype(jnp.float32), (((1,), (1,)), ((), ())), precision=lax.Precision.HIGHEST, preferred_element_type=jnp.float32)
        matrix = matrix - product
        new_strip = jnp.where(below_panel, solved, column_strip)
        new_strip = lax.dynamic_update_slice(new_strip, factor, (offset, zero_index))
        matrix = lax.dynamic_update_slice(matrix, new_strip, (zero_index, offset))
    return matrix.reshape(matrix_in.shape)
```

```python
import functools

import jax
import jax.numpy as jnp
from jax import lax
from jax.experimental import pallas as pl
from jax.experimental.pallas import tpu as pltpu
from jax.sharding import PartitionSpec as P

PANELS = 2
TILE = 128
CORES = 2
MESH = pl.DeviceIdType.MESH
VMEM_LIMIT = 56 * 1024 * 1024
PIECE = 256
GROUPS = 2


def dot(left, right, dims, precision=lax.Precision.HIGHEST):
    return lax.dot_general(
        left, right, (dims, ((), ())), precision=precision,
        preferred_element_type=jnp.float32,
    )


def eliminate(s_ref, o_ref, d_ref):
    order = o_ref.shape[0]
    width = order // PANELS
    tiles = order // TILE
    span = order + TILE
    per = width // TILE
    rows = lax.broadcasted_iota(jnp.int32, (TILE, TILE), 0)
    lanes = lax.broadcasted_iota(jnp.int32, (TILE, TILE), 1)
    row_id = lax.broadcasted_iota(jnp.int32, (TILE, 1), 0)
    lane_id = lax.broadcasted_iota(jnp.int32, (1, TILE), 1)
    eye = jnp.where(rows == lanes, 1.0, 0.0).astype(jnp.float32)

    for t in range(per):
        cols = slice(t * TILE, (t + 1) * TILE)
        far = slice(width + t * TILE, width + (t + 1) * TILE)
        piece = slice(t * width, (t + 1) * width)
        o_ref[:width, cols] = s_ref[0, piece, :]
        o_ref[:width, far] = s_ref[1, piece, :]
        o_ref[width:, far] = s_ref[2, piece, :]
        o_ref[width:, cols] = jnp.zeros((width, TILE), jnp.float32)

    def init(t, _):
        at = pl.ds(pl.multiple_of(t * TILE, TILE), TILE)
        o_ref[at, order:] = jnp.zeros((TILE, order), jnp.float32)
        o_ref[at, pl.ds(pl.multiple_of(order + t * TILE, TILE), TILE)] = eye
        return 0

    lax.fori_loop(0, tiles, init, 0)

    def tile_step(b, _):
        start = pl.multiple_of(b * TILE, TILE)
        at = pl.ds(start, TILE)
        window = pl.ds(start, span)
        d_ref[:, :TILE] = o_ref[at, at]
        d_ref[:, TILE:] = eye

        def pivot(j, _):
            row = d_ref[pl.ds(j, 1), :]
            left = d_ref[:, :TILE]
            diag = jnp.sum(jnp.where(lane_id == j, row[:, :TILE], 0.0), axis=1, keepdims=True)
            col = jnp.sum(jnp.where(lanes == j, left, 0.0), axis=1, keepdims=True)
            inv = 1.0 / jnp.sqrt(diag)
            unit = row * inv
            mult = jnp.where(row_id > j, col * inv, 0.0)
            d_ref[...] = d_ref[...] - mult * unit
            d_ref[pl.ds(j, 1), :] = unit
            return 0

        lax.fori_loop(0, TILE, pivot, 0)
        upper = jnp.where(rows <= lanes, d_ref[:, :TILE], 0.0)
        lower_inv = jnp.where(rows >= lanes, d_ref[:, TILE:], 0.0)
        o_ref[at, window] = dot(lower_inv, o_ref[at, window], ((1,), (0,)))
        o_ref[at, at] = upper

        def below(i, _):
            there = pl.ds(pl.multiple_of(i * TILE, TILE), TILE)
            o_ref[there, window] = o_ref[there, window] - dot(
                o_ref[at, there], o_ref[at, window], ((0,), (0,))
            )
            return 0

        lax.fori_loop(b + 1, tiles, below, 0)
        return 0

    lax.fori_loop(0, tiles, tile_step, 0)


def factor_and_invert(pieces):
    order = PANELS * int(round((pieces.shape[1] * TILE) ** 0.5))
    both = pl.pallas_call(
        eliminate,
        out_shape=jax.ShapeDtypeStruct((order, 2 * order), jnp.float32),
        in_specs=[pl.BlockSpec(memory_space=pltpu.VMEM)],
        out_specs=pl.BlockSpec(memory_space=pltpu.VMEM),
        scratch_shapes=[pltpu.VMEM((TILE, 2 * TILE), jnp.float32)],
        compiler_params=pltpu.CompilerParams(vmem_limit_bytes=40 * 1024 * 1024),
        cost_estimate=pl.CostEstimate(
            flops=20_000_000_000, bytes_accessed=12 * order * order, transcendentals=order
        ),
    )(pieces)
    return both


def distribute(
    rows, cols, owner, skip_rows, skip_cols,
    strip_ref, band_ref, block_ref,
    raw_ref, across_ref, square_ref,
    one_send, one_recv, all_send, all_recv, twin_send,
    row_send, row_recv, pair_send, pair_recv,
    up_send, down_send, side_send, raw_recv, own_sem, strip_buf, band_buf,
):
    me_r = lax.axis_index("row")
    me_c = lax.axis_index("col")
    me = me_r * cols + me_c
    total = rows * cols
    width = strip_ref.shape[1]
    chunk = block_ref.shape[0] // total
    core = me_r % CORES
    twin = me_r + 1 - 2 * core
    row_of = [(owner + s) % rows for s in range(PANELS)]
    col_of = [(owner + s) % cols for s in range(PANELS)]
    pieces = [(row_of[0], col_of[0]), (row_of[0], col_of[1]), (row_of[1], col_of[1])]

    def chunk_rows(d):
        return pl.ds(pl.multiple_of(d * chunk, 8), chunk)

    def first(q, d):
        return pltpu.make_async_remote_copy(
            src_ref=block_ref.at[chunk_rows(d)],
            dst_ref=square_ref.at[q, chunk_rows(d)],
            send_sem=one_send.at[d], recv_sem=one_recv.at[q],
            device_id=(d // cols, d % cols), device_id_type=MESH,
        )

    def first_own(q):
        return pltpu.make_async_copy(
            block_ref.at[chunk_rows(me)], square_ref.at[q, chunk_rows(me)], own_sem.at[0]
        )

    for q, (r, c) in enumerate(pieces):

        @pl.when(me == r * cols + c)
        def _():
            first_own(q).start()

            def send(s, _):
                first(q, (me + s) % total).start()
                return 0

            lax.fori_loop(1, total, send, 0)

    keep_cols = pl.ds(skip_cols * width, band_ref.shape[1] - skip_cols * width)

    def band_at(s):
        return across_ref.at[pl.ds(s * width, width), keep_cols]

    def down(s, y):
        return pltpu.make_async_remote_copy(
            src_ref=band_ref.at[:, keep_cols], dst_ref=band_at(s),
            send_sem=row_send.at[s, y], recv_sem=row_recv.at[s],
            device_id=(y * CORES + row_of[s] % CORES, me_c), device_id_type=MESH,
        )

    def beside(s, source):
        return pltpu.make_async_remote_copy(
            src_ref=source, dst_ref=band_at(s),
            send_sem=pair_send.at[s], recv_sem=pair_recv.at[s],
            device_id=(twin, me_c), device_id_type=MESH,
        )

    def band_in():
        return pltpu.make_async_copy(band_ref.at[:, keep_cols], band_buf, own_sem.at[1])

    def band_out(s):
        return pltpu.make_async_copy(band_buf, band_at(s), own_sem.at[2])

    chips = rows // CORES
    for s in range(PANELS):

        @pl.when(me_r == row_of[s])
        def _():
            for y in range(chips):
                if y != row_of[s] // CORES:
                    down(s, y).start()
            beside(s, band_ref.at[:, keep_cols]).start()
            band_in().start()

    for q, (r, c) in enumerate(pieces):
        home = r * cols + c

        @pl.when(me == home)
        def _():
            first_own(q).wait()

        @pl.when(me != home)
        def _():
            first(q, me).wait_recv()

    half = total // CORES
    mine = (me_r // CORES) * cols + me_c

    def place(u, side):
        row = (u // cols) * CORES + side
        return row, u % cols

    def every(u, source):
        row, col = place(u, core)
        at = chunk_rows(source)
        return pltpu.make_async_remote_copy(
            src_ref=square_ref.at[:, at], dst_ref=square_ref.at[:, at],
            send_sem=all_send.at[u], recv_sem=all_recv.at[source],
            device_id=(row, col), device_id_type=MESH,
        )

    def across_chip(u, side):
        row, col = place(u, side)
        source = row * cols + col
        at = chunk_rows(source)
        return pltpu.make_async_remote_copy(
            src_ref=square_ref.at[:, at], dst_ref=square_ref.at[:, at],
            send_sem=twin_send.at[u], recv_sem=all_recv.at[source],
            device_id=(twin, me_c), device_id_type=MESH,
        )

    def share(s, _):
        every((mine + s) % half, me).start()
        return 0

    lax.fori_loop(1, half, share, 0)
    across_chip(mine, core).start()

    steps = cols // 2
    me_z, me_x = me_c // 2, me_c % 2
    size = PIECE if width % PIECE == 0 else width
    pieces_of_rows = (strip_ref.shape[0] - skip_rows * width) // size

    def rows_at(t):
        return pl.ds(pl.multiple_of(skip_rows * width + t * size, 8), size)

    def carry(s, t, source, sems, col):
        return pltpu.make_async_remote_copy(
            src_ref=source, dst_ref=raw_ref.at[s, rows_at(t)],
            send_sem=sems.at[t], recv_sem=raw_recv.at[s, t],
            device_id=(me_r, col), device_id_type=MESH,
        )

    def lanes_of(s, t, source):
        home = col_of[s] // 2
        return [
            ((me_z >= home) & (me_z < steps - 1), carry(s, t, source, up_send, (me_c + 2) % cols)),
            ((me_z <= home) & (me_z > 0), carry(s, t, source, down_send, (me_c + cols - 2) % cols)),
            (me_z >= 0, carry(s, t, source, side_send, me_c + 1 - 2 * me_x)),
        ]

    keep_rows = pl.ds(skip_rows * width, strip_ref.shape[0] - skip_rows * width)

    def strip_in():
        return pltpu.make_async_copy(strip_ref.at[keep_rows], strip_buf, own_sem.at[3])

    def strip_out(s):
        return pltpu.make_async_copy(strip_buf, raw_ref.at[s, keep_rows], own_sem.at[4])

    for s in range(PANELS):

        @pl.when(me_c == col_of[s])
        def _():
            def send(t, _):
                for needed, copy in lanes_of(s, t, strip_ref.at[rows_at(t)]):
                    pl.when(needed)(copy.start)
                return 0

            lax.fori_loop(0, pieces_of_rows, send, 0)
            strip_in().start()
            strip_in().wait()
            strip_out(s).start()

        @pl.when(me_r == row_of[s])
        def _():
            band_in().wait()
            band_out(s).start()

    def pass_band():
        for s in range(PANELS):

            @pl.when((core == row_of[s] % CORES) & (me_r != row_of[s]))
            def _():
                down(s, 0).wait_recv()
                beside(s, band_at(s)).start()

    def relay(s, _):
        u = (mine + half - s) % half
        row, col = place(u, core)
        every(mine, row * cols + col).wait_recv()
        across_chip(u, core).start()
        return 0

    lax.fori_loop(1, half, relay, 0)

    for s in range(PANELS):

        @pl.when((me_x == col_of[s] % 2) & (me_c != col_of[s]))
        def _():
            def forward(t, _):
                carry(s, t, raw_ref.at[s, rows_at(t)], side_send, me_c).wait_recv()
                for needed, copy in lanes_of(s, t, raw_ref.at[s, rows_at(t)]):
                    pl.when(needed)(copy.start)
                return 0

            lax.fori_loop(0, pieces_of_rows, forward, 0)

    pass_band()

    def from_twin(u, _):
        across_chip(u, 1 - core).wait_recv()
        across_chip(u, core).wait_send()
        return 0

    lax.fori_loop(0, half, from_twin, 0)

    def shared(s, _):
        every((mine + s) % half, me).wait_send()
        return 0

    lax.fori_loop(1, half, shared, 0)

    for q, (r, c) in enumerate(pieces):

        @pl.when(me == r * cols + c)
        def _():
            def sent(s, _):
                first(q, (me + s) % total).wait_send()
                return 0

            lax.fori_loop(1, total, sent, 0)

    for s in range(PANELS):

        @pl.when(me_x == col_of[s] % 2)
        def _():
            def sent(t, _):
                for needed, copy in lanes_of(s, t, strip_ref.at[rows_at(t)]):
                    pl.when(needed)(copy.wait_send)
                return 0

            lax.fori_loop(0, pieces_of_rows, sent, 0)

        @pl.when(me_x != col_of[s] % 2)
        def _():
            def arrive(t, _):
                carry(s, t, raw_ref.at[s, rows_at(t)], side_send, me_c).wait_recv()
                return 0

            lax.fori_loop(0, pieces_of_rows, arrive, 0)

        @pl.when(me_c == col_of[s])
        def _():
            strip_out(s).wait()

        @pl.when(core == row_of[s] % CORES)
        def _():
            beside(s, band_at(s)).wait_send()

        @pl.when(core != row_of[s] % CORES)
        def _():
            beside(s, band_at(s)).wait_recv()

        @pl.when(me_r == row_of[s])
        def _():
            for y in range(chips):
                if y != row_of[s] // CORES:
                    down(s, y).wait_send()
            band_out(s).wait()


def spread_window(rows, cols, variant, strip, band, block):
    width = strip.shape[1]
    total = rows * cols
    loc_rows, loc_cols = strip.shape[0] // width, band.shape[1] // width
    dma = pltpu.SemaphoreType.DMA
    group, owner = divmod(variant, cols)
    lowest = group * (loc_cols // GROUPS) * cols + owner
    skip_rows = min((lowest + 1) // rows, loc_rows - 1)
    skip_cols = min((lowest + 2) // cols, loc_cols - 1)
    size = PIECE if width % PIECE == 0 else width
    parts = max(loc_rows - skip_rows, 1) * width // size
    half = total // CORES
    return pl.pallas_call(
        functools.partial(distribute, rows, cols, owner, skip_rows, skip_cols),
        out_shape=(
            jax.ShapeDtypeStruct((PANELS,) + strip.shape, jnp.float32),
            jax.ShapeDtypeStruct((PANELS * width, band.shape[1]), jnp.float32),
            jax.ShapeDtypeStruct((3,) + block.shape, jnp.float32),
        ),
        in_specs=[pl.BlockSpec(memory_space=pltpu.HBM)] * 3,
        out_specs=[pl.BlockSpec(memory_space=pltpu.HBM)] * 3,
        scratch_shapes=[
            dma((total,)), dma((3,)), dma((half,)), dma((total,)), dma((half,)),
            dma((PANELS, rows // CORES)), dma((PANELS,)), dma((PANELS,)), dma((PANELS,)),
            dma((parts,)), dma((parts,)), dma((parts,)), dma((PANELS, parts)), dma((5,)),
            pltpu.VMEM((strip.shape[0] - skip_rows * width, width), jnp.float32),
            pltpu.VMEM((width, band.shape[1] - skip_cols * width), jnp.float32),
        ],
        compiler_params=pltpu.CompilerParams(
            has_side_effects=True, vmem_limit_bytes=VMEM_LIMIT
        ),
        name="distribute",
    )(strip, band, block)


def prepare(place_ref, inverse_ref, across_ref, high_ref, low_ref, *, cols_dev):
    col_block = pl.program_id(0) * cols_dev + place_ref[2]
    panel = place_ref[0]
    width = across_ref.shape[1]

    def put(weights):
        top = weights.astype(jnp.bfloat16)
        high_ref[...] = top
        low_ref[...] = (weights - top.astype(jnp.float32)).astype(jnp.bfloat16)

    for s in range(PANELS):

        @pl.when(col_block == panel + s)
        def _():
            put(inverse_ref[s * width:(s + 1) * width, :].T)

    @pl.when(col_block >= panel + PANELS)
    def _():
        solved = dot(inverse_ref[...], across_ref[...], ((1,), (0,)))
        put(-dot(inverse_ref[...], solved, ((0,), (0,))))


def column_weights(place, both, across, width, cols_dev):
    order, total = across.shape
    spec = pl.BlockSpec((order, width), lambda j, place: (0, j))
    shape = jax.ShapeDtypeStruct(across.shape, jnp.bfloat16)
    return pl.pallas_call(
        functools.partial(prepare, cols_dev=cols_dev),
        grid_spec=pltpu.PrefetchScalarGridSpec(
            num_scalar_prefetch=1,
            grid=(total // width,),
            in_specs=[
                pl.BlockSpec(
                    (order, order), lambda j, place: (0, 1), pipeline_mode=pl.Buffered(1)
                ),
                spec,
            ],
            out_specs=[spec, spec],
        ),
        out_shape=(shape, shape),
        compiler_params=pltpu.CompilerParams(vmem_limit_bytes=VMEM_LIMIT),
        cost_estimate=pl.CostEstimate(
            flops=24 * order * order * total, bytes_accessed=12 * order * total, transcendentals=0
        ),
        name="prepare",
    )(place, both, across)


def update(place_ref, m_ref, r_ref, special_ref, high_ref, low_ref, diag_ref, o_ref, rh_ref, rl_ref, *, rows_dev, cols_dev, loc_cols):
    panel = place_ref[0]
    row_block = pl.program_id(0) * rows_dev + place_ref[1]
    here = r_ref.shape[1]
    width = high_ref.shape[1] // loc_cols
    lanes = width // TILE
    groups = loc_cols * lanes

    @pl.when(row_block > panel)
    def _():
        for s in range(PANELS):
            at = slice(s * width, (s + 1) * width)
            raw = jnp.where(row_block == panel + 1, special_ref[:, at], r_ref[s])
            top = raw.astype(jnp.bfloat16)
            rh_ref[:, at] = top
            rl_ref[:, at] = (raw - top.astype(jnp.float32)).astype(jnp.bfloat16)

    for j in range(loc_cols):
        col_block = j * cols_dev + place_ref[2]
        last = (row_block == panel + 1) & (col_block == panel + 1)
        first = (row_block == panel) & (col_block == panel)
        active = (row_block > panel) & (col_block >= panel) & jnp.logical_not(last)

        def rows_at(t):
            return pl.ds(t * loc_cols + j, here, stride=groups)

        @pl.when(active)
        def _():
            at = slice(j * width, (j + 1) * width)
            dims = ((1,), (0,))
            acc = dot(rh_ref[...], high_ref[:, at], dims, None)
            acc += dot(rh_ref[...], low_ref[:, at], dims, None)
            acc += dot(rl_ref[...], high_ref[:, at], dims, None)
            keep = jnp.where(col_block > panel + 1, 1.0, 0.0).astype(jnp.float32)
            for t in range(lanes):
                o_ref[0, rows_at(t), :] = (
                    m_ref[0, rows_at(t), :] * keep + acc[:, t * TILE:(t + 1) * TILE]
                )

        @pl.when(jnp.logical_not(active))
        def _():
            for t in range(lanes):
                o_ref[0, rows_at(t), :] = m_ref[0, rows_at(t), :]

        @pl.when(first | last)
        def _():
            for t in range(lanes):
                o_ref[0, rows_at(t), :] = diag_ref[0, :, t * TILE:(t + 1) * TILE]


def apply_update(place, matrix, raw_rows, special, high, low, diag, rows_dev, cols_dev):
    loc_rows, width, loc_cols, _unused = matrix.shape
    lanes = width // TILE
    groups = loc_cols * lanes
    step = min(width, 256)
    flat = matrix.reshape(loc_rows, width, loc_cols, lanes, TILE)
    flat = flat.transpose(0, 1, 3, 2, 4).reshape(loc_rows, width * groups, TILE)
    inner = high.shape[0]
    cut = width // step
    out = pl.pallas_call(
        functools.partial(update, rows_dev=rows_dev, cols_dev=cols_dev, loc_cols=loc_cols),
        grid_spec=pltpu.PrefetchScalarGridSpec(
            num_scalar_prefetch=1,
            grid=(loc_rows, cut),
            in_specs=[
                pl.BlockSpec((1, step * groups, TILE), lambda i, q, place: (i, q, 0)),
                pl.BlockSpec((PANELS, step, width), lambda i, q, place: (0, i * cut + q, 0)),
                pl.BlockSpec((step, inner), lambda i, q, place: (q, 0)),
                pl.BlockSpec(high.shape, lambda i, q, place: (0, 0), pipeline_mode=pl.Buffered(1)),
                pl.BlockSpec(low.shape, lambda i, q, place: (0, 0), pipeline_mode=pl.Buffered(1)),
                pl.BlockSpec(
                    (1, step, width),
                    lambda i, q, place: (
                        jnp.where(i * rows_dev + place[1] == place[0] + 1, 1, 0), q, 0
                    ),
                ),
            ],
            out_specs=pl.BlockSpec((1, step * groups, TILE), lambda i, q, place: (i, q, 0)),
            scratch_shapes=[
                pltpu.VMEM((step, inner), jnp.bfloat16),
                pltpu.VMEM((step, inner), jnp.bfloat16),
            ],
        ),
        out_shape=jax.ShapeDtypeStruct(flat.shape, jnp.float32),
        compiler_params=pltpu.CompilerParams(vmem_limit_bytes=VMEM_LIMIT),
        cost_estimate=pl.CostEstimate(
            flops=60_000_000_000, bytes_accessed=8 * matrix.size, transcendentals=0
        ),
        name="update",
    )(place, flat, raw_rows, special, high, low, diag)
    out = out.reshape(loc_rows, width, lanes, loc_cols, TILE).transpose(0, 1, 3, 2, 4)
    return out.reshape(matrix.shape)


def per_device(matrix, panel_start):
    rows_dev = lax.axis_size("row")
    cols_dev = lax.axis_size("col")
    my_row = lax.axis_index("row")
    my_col = lax.axis_index("col")
    loc_rows, width, loc_cols, _unused = matrix.shape
    panel = panel_start[0]
    later = panel + 1

    own_col = jnp.where(my_col == panel % cols_dev, panel // cols_dev, later // cols_dev)
    own_row = jnp.where(my_row == panel % rows_dev, panel // rows_dev, later // rows_dev)
    strip = lax.dynamic_index_in_dim(matrix, own_col, 2, keepdims=False)
    band = lax.dynamic_index_in_dim(matrix, own_row, 0, keepdims=False)
    block = lax.dynamic_index_in_dim(strip, own_row, 0, keepdims=False)
    strip = strip.reshape(loc_rows * width, width)
    band = band.reshape(width, loc_cols * width)
    block = block.reshape(width, width // TILE, TILE).transpose(1, 0, 2).reshape(-1, TILE)

    group = panel // (loc_cols // GROUPS * cols_dev)
    raw_rows, across, pieces = lax.switch(
        group * cols_dev + panel % cols_dev,
        [
            functools.partial(spread_window, rows_dev, cols_dev, v)
            for v in range(GROUPS * cols_dev)
        ],
        strip, band, block,
    )

    both = factor_and_invert(pieces)
    order = PANELS * width
    upper = both[:, :order]
    diag = jnp.stack([
        jnp.tril(upper[at, at].T) for at in (slice(0, width), slice(width, order))
    ])
    cross = upper[:width, width:]
    lanes = width // TILE
    beside = pieces[1].reshape(lanes, width, TILE).transpose(0, 2, 1).reshape(width, width)
    special = jnp.concatenate([beside, dot(cross, cross, ((0,), (0,)))], axis=1)
    place = jnp.stack([panel, my_row, my_col]).astype(jnp.int32)
    high, low = column_weights(place, both, across, width, cols_dev)
    return apply_update(
        place, matrix, raw_rows, special, high, low, diag, rows_dev, cols_dev
    )


def solution(mesh):
    return jax.shard_map(
        per_device,
        mesh=mesh,
        in_specs=(P(None, "row", None, "col"), P()),
        out_specs=P(None, "row", None, "col"),
        check_vma=False,
    )
```

```python
import functools

import jax
import jax.numpy as jnp
from jax import lax
from jax.experimental import pallas as pl
from jax.experimental.pallas import tpu as pltpu
from jax.sharding import PartitionSpec as P

PANELS = 2
TILE = 128
CORES = 2
MESH = pl.DeviceIdType.MESH
VMEM_LIMIT = 56 * 1024 * 1024
PIECE = 128
RUN = 16
GROUPS = 2


def dot(left, right, dims, precision=lax.Precision.HIGHEST):
    return lax.dot_general(
        left, right, (dims, ((), ())), precision=precision,
        preferred_element_type=jnp.float32,
    )


def eliminate(s_ref, o_ref, d_ref, slot):
    order = o_ref.shape[0]
    width = order // PANELS
    tiles = order // TILE
    span = order + TILE
    per = width // TILE
    rows = lax.broadcasted_iota(jnp.int32, (TILE, TILE), 0)
    lanes = lax.broadcasted_iota(jnp.int32, (TILE, TILE), 1)
    row_id = lax.broadcasted_iota(jnp.int32, (TILE, 1), 0)
    lane_id = lax.broadcasted_iota(jnp.int32, (1, TILE), 1)
    eye = jnp.where(rows == lanes, 1.0, 0.0).astype(jnp.float32)

    for t in range(per):
        cols = slice(t * TILE, (t + 1) * TILE)
        far = slice(width + t * TILE, width + (t + 1) * TILE)
        piece = slice(t * width, (t + 1) * width)
        o_ref[:width, cols] = s_ref[0, piece, :]
        o_ref[:width, far] = s_ref[1, piece, :]
        o_ref[width:, far] = s_ref[2, piece, :]
        o_ref[width:, cols] = jnp.zeros((width, TILE), jnp.float32)

    def init(t, _):
        at = pl.ds(pl.multiple_of(t * TILE, TILE), TILE)
        o_ref[at, order:] = jnp.zeros((TILE, order), jnp.float32)
        o_ref[at, pl.ds(pl.multiple_of(order + t * TILE, TILE), TILE)] = eye
        return 0

    lax.fori_loop(0, tiles, init, 0)

    def tile_step(b, _):
        start = pl.multiple_of(b * TILE, TILE)
        at = pl.ds(start, TILE)
        window = pl.ds(start, span)
        d_ref[:, :TILE] = o_ref[at, at]
        d_ref[:, TILE:] = eye

        def pivot(j, _):
            row = d_ref[pl.ds(j, 1), :]
            left = d_ref[:, :TILE]
            diag = jnp.sum(jnp.where(lane_id == j, row[:, :TILE], 0.0), axis=1, keepdims=True)
            col = jnp.sum(jnp.where(lanes == j, left, 0.0), axis=1, keepdims=True)
            inv = 1.0 / jnp.sqrt(diag)
            unit = row * inv
            mult = jnp.where(row_id > j, col * inv, 0.0)
            d_ref[...] = d_ref[...] - mult * unit
            d_ref[pl.ds(j, 1), :] = unit
            return 0

        def stretch(part, _):
            lax.fori_loop(part * RUN, (part + 1) * RUN, pivot, 0)
            slot(b * (TILE // RUN) + part)
            return 0

        lax.fori_loop(0, TILE // RUN, stretch, 0)
        upper = jnp.where(rows <= lanes, d_ref[:, :TILE], 0.0)
        lower_inv = jnp.where(rows >= lanes, d_ref[:, TILE:], 0.0)
        o_ref[at, window] = dot(lower_inv, o_ref[at, window], ((1,), (0,)))
        o_ref[at, at] = upper

        def below(i, _):
            there = pl.ds(pl.multiple_of(i * TILE, TILE), TILE)
            o_ref[there, window] = o_ref[there, window] - dot(
                o_ref[at, there], o_ref[at, window], ((0,), (0,))
            )
            return 0

        lax.fori_loop(b + 1, tiles, below, 0)
        return 0

    lax.fori_loop(0, tiles, tile_step, 0)


def distribute(
    rows, cols, owner, skip_rows, skip_cols,
    strip_ref, band_ref, block_ref,
    raw_ref, across_ref, square_ref, both_ref,
    one_send, one_recv, all_send, all_recv, twin_send,
    row_send, row_recv, pair_send, pair_recv,
    up_send, down_send, side_send, raw_recv, own_sem, strip_buf, band_buf, square_buf, tile_buf,
):
    me_r = lax.axis_index("row")
    me_c = lax.axis_index("col")
    me = me_r * cols + me_c
    total = rows * cols
    width = strip_ref.shape[1]
    chunk = block_ref.shape[0] // total
    core = me_r % CORES
    twin = me_r + 1 - 2 * core
    row_of = [(owner + s) % rows for s in range(PANELS)]
    col_of = [(owner + s) % cols for s in range(PANELS)]
    pieces = [(row_of[0], col_of[0]), (row_of[0], col_of[1]), (row_of[1], col_of[1])]

    def chunk_rows(d):
        return pl.ds(pl.multiple_of(d * chunk, 8), chunk)

    def first(q, d):
        return pltpu.make_async_remote_copy(
            src_ref=block_ref.at[chunk_rows(d)],
            dst_ref=square_ref.at[q, chunk_rows(d)],
            send_sem=one_send.at[d], recv_sem=one_recv.at[q],
            device_id=(d // cols, d % cols), device_id_type=MESH,
        )

    def first_own(q):
        return pltpu.make_async_copy(
            block_ref.at[chunk_rows(me)], square_ref.at[q, chunk_rows(me)], own_sem.at[0]
        )

    for q, (r, c) in enumerate(pieces):

        @pl.when(me == r * cols + c)
        def _():
            first_own(q).start()

            def send(s, _):
                first(q, (me + s) % total).start()
                return 0

            lax.fori_loop(1, total, send, 0)

    keep_cols = pl.ds(skip_cols * width, band_ref.shape[1] - skip_cols * width)

    def band_at(s):
        return across_ref.at[pl.ds(s * width, width), keep_cols]

    def down(s, y):
        return pltpu.make_async_remote_copy(
            src_ref=band_ref.at[:, keep_cols], dst_ref=band_at(s),
            send_sem=row_send.at[s, y], recv_sem=row_recv.at[s],
            device_id=(y * CORES + row_of[s] % CORES, me_c), device_id_type=MESH,
        )

    def beside(s, source):
        return pltpu.make_async_remote_copy(
            src_ref=source, dst_ref=band_at(s),
            send_sem=pair_send.at[s], recv_sem=pair_recv.at[s],
            device_id=(twin, me_c), device_id_type=MESH,
        )

    def band_in():
        return pltpu.make_async_copy(band_ref.at[:, keep_cols], band_buf, own_sem.at[1])

    def band_out(s):
        return pltpu.make_async_copy(band_buf, band_at(s), own_sem.at[2])

    chips = rows // CORES
    for s in range(PANELS):

        @pl.when(me_r == row_of[s])
        def _():
            for y in range(chips):
                if y != row_of[s] // CORES:
                    down(s, y).start()
            beside(s, band_ref.at[:, keep_cols]).start()
            band_in().start()

    for q, (r, c) in enumerate(pieces):
        home = r * cols + c

        @pl.when(me == home)
        def _():
            first_own(q).wait()

        @pl.when(me != home)
        def _():
            first(q, me).wait_recv()

    half = total // CORES
    mine = (me_r // CORES) * cols + me_c

    def place(u, side):
        row = (u // cols) * CORES + side
        return row, u % cols

    def every(u, source):
        row, col = place(u, core)
        at = chunk_rows(source)
        return pltpu.make_async_remote_copy(
            src_ref=square_ref.at[:, at], dst_ref=square_ref.at[:, at],
            send_sem=all_send.at[u], recv_sem=all_recv.at[source],
            device_id=(row, col), device_id_type=MESH,
        )

    def across_chip(u, side):
        row, col = place(u, side)
        source = row * cols + col
        at = chunk_rows(source)
        return pltpu.make_async_remote_copy(
            src_ref=square_ref.at[:, at], dst_ref=square_ref.at[:, at],
            send_sem=twin_send.at[u], recv_sem=all_recv.at[source],
            device_id=(twin, me_c), device_id_type=MESH,
        )

    def share(s, _):
        every((mine + s) % half, me).start()
        return 0

    lax.fori_loop(1, half, share, 0)
    across_chip(mine, core).start()

    steps = cols // 2
    me_z, me_x = me_c // 2, me_c % 2
    size = PIECE if width % PIECE == 0 else width
    pieces_of_rows = (strip_ref.shape[0] - skip_rows * width) // size

    def rows_at(t):
        return pl.ds(pl.multiple_of(skip_rows * width + t * size, 8), size)

    def carry(s, t, source, sems, col):
        return pltpu.make_async_remote_copy(
            src_ref=source, dst_ref=raw_ref.at[s, rows_at(t)],
            send_sem=sems.at[t], recv_sem=raw_recv.at[s, t],
            device_id=(me_r, col), device_id_type=MESH,
        )

    def lanes_of(s, t, source):
        home = col_of[s] // 2
        return [
            ((me_z >= home) & (me_z < steps - 1), carry(s, t, source, up_send, (me_c + 2) % cols)),
            ((me_z <= home) & (me_z > 0), carry(s, t, source, down_send, (me_c + cols - 2) % cols)),
            (me_z >= 0, carry(s, t, source, side_send, me_c + 1 - 2 * me_x)),
        ]

    keep_rows = pl.ds(skip_rows * width, strip_ref.shape[0] - skip_rows * width)

    def strip_in():
        return pltpu.make_async_copy(strip_ref.at[keep_rows], strip_buf, own_sem.at[3])

    def strip_out(s):
        return pltpu.make_async_copy(strip_buf, raw_ref.at[s, keep_rows], own_sem.at[4])

    for s in range(PANELS):

        @pl.when(me_c == col_of[s])
        def _():
            def send(t, _):
                for needed, copy in lanes_of(s, t, strip_ref.at[rows_at(t)]):
                    pl.when(needed)(copy.start)
                return 0

            lax.fori_loop(0, pieces_of_rows, send, 0)
            strip_in().start()
            strip_in().wait()
            strip_out(s).start()

        @pl.when(me_r == row_of[s])
        def _():
            band_in().wait()
            band_out(s).start()

    def pass_band():
        for s in range(PANELS):

            @pl.when((core == row_of[s] % CORES) & (me_r != row_of[s]))
            def _():
                down(s, 0).wait_recv()
                beside(s, band_at(s)).start()

    def relay(s, _):
        u = (mine + half - s) % half
        row, col = place(u, core)
        every(mine, row * cols + col).wait_recv()
        across_chip(u, core).start()
        return 0

    lax.fori_loop(1, half, relay, 0)

    def from_twin(u, _):
        across_chip(u, 1 - core).wait_recv()
        across_chip(u, core).wait_send()
        return 0

    lax.fori_loop(0, half, from_twin, 0)
    load = pltpu.make_async_copy(square_ref, square_buf, own_sem.at[0])
    load.start()
    load.wait()

    tiles = both_ref.shape[0] // TILE
    slots = tiles * (TILE // RUN)

    def hops(s):
        return jnp.abs(me_z - col_of[s] // 2)

    def on_line(s):
        return (me_x == col_of[s] % 2) & (me_c != col_of[s])

    def forward(s, t):
        carry(s, t, raw_ref.at[s, rows_at(t)], side_send, me_c).wait_recv()
        for needed, copy in lanes_of(s, t, raw_ref.at[s, rows_at(t)]):
            pl.when(needed)(copy.start)

    def slot(n):
        for s in range(PANELS):
            since = n - 3 * hops(s)
            t = (2 * since + 4) // 5

            @pl.when(
                on_line(s) & (since >= 0) & ((5 * t) // 2 == since) & (t < pieces_of_rows)
            )
            def _():
                forward(s, t)

        pl.when(n == slots * 3 // 4)(pass_band)

    eliminate(square_buf, both_ref, tile_buf, slot)

    for s in range(PANELS):

        @pl.when(on_line(s))
        def _():
            done = (2 * (slots - 1 - 3 * hops(s)) + 1) // 5 + 1

            def late(t, _):
                forward(s, t)
                return 0

            lax.fori_loop(jnp.minimum(done, pieces_of_rows), pieces_of_rows, late, 0)

    def shared(s, _):
        every((mine + s) % half, me).wait_send()
        return 0

    lax.fori_loop(1, half, shared, 0)

    for q, (r, c) in enumerate(pieces):

        @pl.when(me == r * cols + c)
        def _():
            def sent(s, _):
                first(q, (me + s) % total).wait_send()
                return 0

            lax.fori_loop(1, total, sent, 0)

    for s in range(PANELS):

        @pl.when(me_x == col_of[s] % 2)
        def _():
            def sent(t, _):
                for needed, copy in lanes_of(s, t, strip_ref.at[rows_at(t)]):
                    pl.when(needed)(copy.wait_send)
                return 0

            lax.fori_loop(0, pieces_of_rows, sent, 0)

        @pl.when(me_x != col_of[s] % 2)
        def _():
            def arrive(t, _):
                carry(s, t, raw_ref.at[s, rows_at(t)], side_send, me_c).wait_recv()
                return 0

            lax.fori_loop(0, pieces_of_rows, arrive, 0)

        @pl.when(me_c == col_of[s])
        def _():
            strip_out(s).wait()

        @pl.when(core == row_of[s] % CORES)
        def _():
            beside(s, band_at(s)).wait_send()

        @pl.when(core != row_of[s] % CORES)
        def _():
            beside(s, band_at(s)).wait_recv()

        @pl.when(me_r == row_of[s])
        def _():
            for y in range(chips):
                if y != row_of[s] // CORES:
                    down(s, y).wait_send()
            band_out(s).wait()


def spread_window(rows, cols, variant, strip, band, block):
    width = strip.shape[1]
    total = rows * cols
    loc_rows, loc_cols = strip.shape[0] // width, band.shape[1] // width
    dma = pltpu.SemaphoreType.DMA
    group, owner = divmod(variant, cols)
    lowest = group * (loc_cols // GROUPS) * cols + owner
    skip_rows = min((lowest + 1) // rows, loc_rows - 1)
    skip_cols = min((lowest + 2) // cols, loc_cols - 1)
    size = PIECE if width % PIECE == 0 else width
    parts = max(loc_rows - skip_rows, 1) * width // size
    half = total // CORES
    return pl.pallas_call(
        functools.partial(distribute, rows, cols, owner, skip_rows, skip_cols),
        out_shape=(
            jax.ShapeDtypeStruct((PANELS,) + strip.shape, jnp.float32),
            jax.ShapeDtypeStruct((PANELS * width, band.shape[1]), jnp.float32),
            jax.ShapeDtypeStruct((3,) + block.shape, jnp.float32),
            jax.ShapeDtypeStruct((PANELS * width, 2 * PANELS * width), jnp.float32),
        ),
        in_specs=[pl.BlockSpec(memory_space=pltpu.HBM)] * 3,
        out_specs=[pl.BlockSpec(memory_space=pltpu.HBM)] * 3
        + [pl.BlockSpec(memory_space=pltpu.VMEM)],
        scratch_shapes=[
            dma((total,)), dma((3,)), dma((half,)), dma((total,)), dma((half,)),
            dma((PANELS, rows // CORES)), dma((PANELS,)), dma((PANELS,)), dma((PANELS,)),
            dma((parts,)), dma((parts,)), dma((parts,)), dma((PANELS, parts)), dma((5,)),
            pltpu.VMEM((strip.shape[0] - skip_rows * width, width), jnp.float32),
            pltpu.VMEM((width, band.shape[1] - skip_cols * width), jnp.float32),
            pltpu.VMEM((3,) + block.shape, jnp.float32),
            pltpu.VMEM((TILE, 2 * TILE), jnp.float32),
        ],
        compiler_params=pltpu.CompilerParams(
            has_side_effects=True, vmem_limit_bytes=VMEM_LIMIT
        ),
        name="distribute",
    )(strip, band, block)


def prepare(place_ref, inverse_ref, across_ref, high_ref, low_ref, *, cols_dev):
    col_block = pl.program_id(0) * cols_dev + place_ref[2]
    panel = place_ref[0]
    width = across_ref.shape[1]

    def put(weights):
        top = weights.astype(jnp.bfloat16)
        high_ref[...] = top
        low_ref[...] = (weights - top.astype(jnp.float32)).astype(jnp.bfloat16)

    for s in range(PANELS):

        @pl.when(col_block == panel + s)
        def _():
            put(inverse_ref[s * width:(s + 1) * width, :].T)

    @pl.when(col_block >= panel + PANELS)
    def _():
        solved = dot(inverse_ref[...], across_ref[...], ((1,), (0,)))
        put(-dot(inverse_ref[...], solved, ((0,), (0,))))


def column_weights(place, both, across, width, cols_dev):
    order, total = across.shape
    spec = pl.BlockSpec((order, width), lambda j, place: (0, j))
    shape = jax.ShapeDtypeStruct(across.shape, jnp.bfloat16)
    return pl.pallas_call(
        functools.partial(prepare, cols_dev=cols_dev),
        grid_spec=pltpu.PrefetchScalarGridSpec(
            num_scalar_prefetch=1,
            grid=(total // width,),
            in_specs=[
                pl.BlockSpec(
                    (order, order), lambda j, place: (0, 1), pipeline_mode=pl.Buffered(1)
                ),
                spec,
            ],
            out_specs=[spec, spec],
        ),
        out_shape=(shape, shape),
        compiler_params=pltpu.CompilerParams(vmem_limit_bytes=VMEM_LIMIT),
        cost_estimate=pl.CostEstimate(
            flops=24 * order * order * total, bytes_accessed=12 * order * total, transcendentals=0
        ),
        name="prepare",
    )(place, both, across)


def update(place_ref, m_ref, r_ref, special_ref, high_ref, low_ref, diag_ref, o_ref, rh_ref, rl_ref, *, rows_dev, cols_dev, loc_cols):
    panel = place_ref[0]
    row_block = pl.program_id(0) * rows_dev + place_ref[1]
    here = r_ref.shape[1]
    width = high_ref.shape[1] // loc_cols
    lanes = width // TILE
    groups = loc_cols * lanes

    @pl.when(row_block > panel)
    def _():
        for s in range(PANELS):
            at = slice(s * width, (s + 1) * width)
            raw = jnp.where(row_block == panel + 1, special_ref[:, at], r_ref[s])
            top = raw.astype(jnp.bfloat16)
            rh_ref[:, at] = top
            rl_ref[:, at] = (raw - top.astype(jnp.float32)).astype(jnp.bfloat16)

    for j in range(loc_cols):
        col_block = j * cols_dev + place_ref[2]
        last = (row_block == panel + 1) & (col_block == panel + 1)
        first = (row_block == panel) & (col_block == panel)
        active = (row_block > panel) & (col_block >= panel) & jnp.logical_not(last)

        def rows_at(t):
            return pl.ds(t * loc_cols + j, here, stride=groups)

        @pl.when(active)
        def _():
            at = slice(j * width, (j + 1) * width)
            dims = ((1,), (0,))
            acc = dot(rh_ref[...], high_ref[:, at], dims, None)
            acc += dot(rh_ref[...], low_ref[:, at], dims, None)
            acc += dot(rl_ref[...], high_ref[:, at], dims, None)
            keep = jnp.where(col_block > panel + 1, 1.0, 0.0).astype(jnp.float32)
            for t in range(lanes):
                o_ref[0, rows_at(t), :] = (
                    m_ref[0, rows_at(t), :] * keep + acc[:, t * TILE:(t + 1) * TILE]
                )

        @pl.when(jnp.logical_not(active))
        def _():
            for t in range(lanes):
                o_ref[0, rows_at(t), :] = m_ref[0, rows_at(t), :]

        @pl.when(first | last)
        def _():
            for t in range(lanes):
                o_ref[0, rows_at(t), :] = diag_ref[0, :, t * TILE:(t + 1) * TILE]


def apply_update(place, matrix, raw_rows, special, high, low, diag, rows_dev, cols_dev):
    loc_rows, width, loc_cols, _unused = matrix.shape
    lanes = width // TILE
    groups = loc_cols * lanes
    step = min(width, 256)
    flat = matrix.reshape(loc_rows, width, loc_cols, lanes, TILE)
    flat = flat.transpose(0, 1, 3, 2, 4).reshape(loc_rows, width * groups, TILE)
    inner = high.shape[0]
    cut = width // step
    out = pl.pallas_call(
        functools.partial(update, rows_dev=rows_dev, cols_dev=cols_dev, loc_cols=loc_cols),
        grid_spec=pltpu.PrefetchScalarGridSpec(
            num_scalar_prefetch=1,
            grid=(loc_rows, cut),
            in_specs=[
                pl.BlockSpec((1, step * groups, TILE), lambda i, q, place: (i, q, 0)),
                pl.BlockSpec((PANELS, step, width), lambda i, q, place: (0, i * cut + q, 0)),
                pl.BlockSpec((step, inner), lambda i, q, place: (q, 0)),
                pl.BlockSpec(high.shape, lambda i, q, place: (0, 0), pipeline_mode=pl.Buffered(1)),
                pl.BlockSpec(low.shape, lambda i, q, place: (0, 0), pipeline_mode=pl.Buffered(1)),
                pl.BlockSpec(
                    (1, step, width),
                    lambda i, q, place: (
                        jnp.where(i * rows_dev + place[1] == place[0] + 1, 1, 0), q, 0
                    ),
                ),
            ],
            out_specs=pl.BlockSpec((1, step * groups, TILE), lambda i, q, place: (i, q, 0)),
            scratch_shapes=[
                pltpu.VMEM((step, inner), jnp.bfloat16),
                pltpu.VMEM((step, inner), jnp.bfloat16),
            ],
        ),
        out_shape=jax.ShapeDtypeStruct(flat.shape, jnp.float32),
        compiler_params=pltpu.CompilerParams(vmem_limit_bytes=VMEM_LIMIT),
        cost_estimate=pl.CostEstimate(
            flops=60_000_000_000, bytes_accessed=8 * matrix.size, transcendentals=0
        ),
        name="update",
    )(place, flat, raw_rows, special, high, low, diag)
    out = out.reshape(loc_rows, width, lanes, loc_cols, TILE).transpose(0, 1, 3, 2, 4)
    return out.reshape(matrix.shape)


def per_device(matrix, panel_start):
    rows_dev = lax.axis_size("row")
    cols_dev = lax.axis_size("col")
    my_row = lax.axis_index("row")
    my_col = lax.axis_index("col")
    loc_rows, width, loc_cols, _unused = matrix.shape
    panel = panel_start[0]
    later = panel + 1

    own_col = jnp.where(my_col == panel % cols_dev, panel // cols_dev, later // cols_dev)
    own_row = jnp.where(my_row == panel % rows_dev, panel // rows_dev, later // rows_dev)
    strip = lax.dynamic_index_in_dim(matrix, own_col, 2, keepdims=False)
    band = lax.dynamic_index_in_dim(matrix, own_row, 0, keepdims=False)
    block = lax.dynamic_index_in_dim(strip, own_row, 0, keepdims=False)
    strip = strip.reshape(loc_rows * width, width)
    band = band.reshape(width, loc_cols * width)
    block = block.reshape(width, width // TILE, TILE).transpose(1, 0, 2).reshape(-1, TILE)

    group = panel // (loc_cols // GROUPS * cols_dev)
    raw_rows, across, pieces, both = lax.switch(
        group * cols_dev + panel % cols_dev,
        [
            functools.partial(spread_window, rows_dev, cols_dev, v)
            for v in range(GROUPS * cols_dev)
        ],
        strip, band, block,
    )

    order = PANELS * width
    upper = both[:, :order]
    diag = jnp.stack([
        jnp.tril(lax.optimization_barrier(upper[at, at]).T)
        for at in (slice(0, width), slice(width, order))
    ])
    cross = upper[:width, width:]
    lanes = width // TILE
    beside = pieces[1].reshape(lanes, width, TILE).transpose(0, 2, 1).reshape(width, width)
    special = jnp.concatenate([beside, dot(cross, cross, ((0,), (0,)))], axis=1)
    place = jnp.stack([panel, my_row, my_col]).astype(jnp.int32)
    high, low = column_weights(place, both, across, width, cols_dev)
    return apply_update(
        place, matrix, raw_rows, special, high, low, diag, rows_dev, cols_dev
    )


def solution(mesh):
    return jax.shard_map(
        per_device,
        mesh=mesh,
        in_specs=(P(None, "row", None, "col"), P()),
        out_specs=P(None, "row", None, "col"),
        check_vma=False,
    )
```
